128 devices in a mesh: pair: 8 (over x, core), row: 16 (over z, y).
Axes of the slice: x: 4, y: 4, z: 4, core: 2. Of those that a mesh axis runs over, the one named last changes fastest.
Arguments:
- descriptors: bfloat16 [64, 2048, 256], P('pair', 'row'), parts along dimension 0, may hold values from -8 to 8
- counts: int32 [64], P('pair'), parts along dimension 0, may hold values from 512 to 2048
- pairs: int32 [32, 2], P('pair'), parts along dimension 0, may hold values from 0 to 7, as said below
- bin_score: float32 [1], replicated, may hold values from 0.5 to 2
Outputs:
- log_match: float32 [32, 2048, 2048], P('pair', 'row'), parts along dimension 0
- row_bins: float32 [32, 2048], P('pair', 'row'), parts along dimension 0
- col_bins: float32 [32, 2048], P('pair'), parts along dimension 0
The draws below stay inside these ranges and needn't reach their ends.
There are 8 independent parts, one for each index of `pair`. The reference program is written for one: setup_inputs(seed, part) draws one part's arguments, and reference() takes and returns one part's arrays. A program takes and returns all parts, laid end to end along the dimension named above; an argument that names none is the same for every part. Nothing has to cross between parts.
Inputs may be any that keep to these rules, and one draw needn't show every extreme that they name: Image k's keypoints are its first counts[k] slots. `pairs`: the two images of a pair differ.
All inputs are finite; a program needn't handle non-finite values.
Results may differ from the reference program's by a relative error of at most 0.0003.
Values may be sent and summed in bfloat16 or wider, within the bound.
A program may use at most 64 MiB of HBM per device.

```python
import jax
import jax.numpy as jnp
from jax import lax

PAIRS = 4
IMAGES = 8
KP = 2048
D = 256
ITERS = 10


def draw_descriptors(key, part):
    values = 2.0 * jax.random.truncated_normal(jax.random.fold_in(key, 5), -4.0, 4.0, (IMAGES, KP, D), jnp.float32)
    return values.astype(jnp.bfloat16)


def draw_pairs(key, part):
    first_image = jax.random.randint(jax.random.fold_in(key, 1), (PAIRS,), 0, IMAGES)
    stride = jax.random.randint(jax.random.fold_in(key, 2), (PAIRS,), 1, IMAGES)
    second_image = (first_image + stride) % IMAGES
    return jnp.stack([first_image, second_image], axis=1).astype(jnp.int32)


def set_ends(entries, key, least, largest):
    spot = [jax.random.randint(jax.random.fold_in(key, axis), (), 0, length) for axis, length in enumerate(entries.shape)]
    longest = entries.shape.index(max(entries.shape))
    neighbour = spot[:longest] + [(spot[longest] + 1) % entries.shape[longest]] + spot[longest + 1:]
    return entries.at[tuple(spot)].set(least).at[tuple(neighbour)].set(largest)


def setup_inputs(seed: int = 0, part: int = 0) -> dict:
    keys = jax.random.split(jax.random.key(seed), 5)
    part_splits = jax.random.split(jax.random.fold_in(keys[4], part), 5)
    descriptors = draw_descriptors(jax.random.fold_in(jax.random.fold_in(keys[4], part), 71), part)
    counts = set_ends(jax.random.randint(part_splits[1], (IMAGES,), KP // 4, KP + 1), jax.random.fold_in(part_splits[1], 1), KP // 4, KP).astype(jnp.int32)
    pairs = draw_pairs(jax.random.fold_in(jax.random.fold_in(keys[4], part), 71), part)
    bin_score = jnp.clip(jax.random.uniform(keys[3], (1,), jnp.float32, 0.5, 2.0), 0.5, 2.0)
    return dict(descriptors=descriptors, counts=counts, pairs=pairs, bin_score=bin_score)


NEG = -1.0e30


def masked_lse(values, kept, reduce_dim):
    held = jnp.where(kept, values, NEG)
    ceiling = jnp.max(held, axis=reduce_dim, keepdims=True)
    summed = jnp.sum(jnp.where(kept, jnp.exp(held - ceiling), 0.0), axis=reduce_dim, keepdims=True)
    return jnp.squeeze(ceiling + jnp.log(summed), reduce_dim)


def reference(descriptors, counts, pairs, bin_score):
    bin_value = bin_score[0]
    row_images = descriptors[pairs[:, 0]]
    col_images = descriptors[pairs[:, 1]]
    row_counts = counts[pairs[:, 0]]
    col_counts = counts[pairs[:, 1]]

    def one_pair(operands):
        row_desc, col_desc, n_rows, n_cols = operands
        scores = jnp.dot(row_desc, col_desc.T, preferred_element_type=jnp.float32) * (D ** -0.5)
        side_line = jnp.zeros((KP, 1), jnp.float32) + bin_value
        upper = jnp.concatenate([scores, side_line], axis=1)
        bin_line = jnp.zeros((1, KP + 1), jnp.float32) + bin_value
        couplings = jnp.concatenate([upper, bin_line], axis=0)
        cell_index = jnp.arange(KP + 1, dtype=jnp.int32)
        row_kept = (cell_index < n_rows) | (cell_index == KP)
        col_kept = (cell_index < n_cols) | (cell_index == KP)
        row_count = n_rows.astype(jnp.float32)
        col_count = n_cols.astype(jnp.float32)
        log_norm = -jnp.log(row_count + col_count)
        log_mu = jnp.where(cell_index == KP, jnp.log(col_count) + log_norm, log_norm)
        log_nu = jnp.where(cell_index == KP, jnp.log(row_count) + log_norm, log_norm)
        row_pot = jnp.zeros((KP + 1,), jnp.float32)
        col_pot = jnp.zeros((KP + 1,), jnp.float32)
        for sweep_index in range(ITERS):
            row_pot = log_mu - masked_lse(couplings + col_pot[None, :], col_kept[None, :], 1)
            col_pot = log_nu - masked_lse(couplings + row_pot[:, None], row_kept[:, None], 0)
        assign = couplings + row_pot[:, None] + col_pot[None, :] - log_norm
        assign = jnp.where(row_kept[:, None] & col_kept[None, :], assign, 0.0)
        return assign[:KP, :KP], assign[:KP, KP], assign[KP, :KP]

    log_match, row_bins, col_bins = lax.map(one_pair, (row_images, col_images, row_counts, col_counts))
    return (log_match, row_bins, col_bins)
```

```python
import functools

import jax
import jax.numpy as jnp
from jax import lax
from jax.experimental import pallas as pl
from jax.experimental.pallas import tpu as pltpu
from jax.sharding import Mesh
from jax.sharding import PartitionSpec as P

D = 256
ITERS = 10
KP = 2048
B = 128
W = KP + 128
CHUNKS = W // 128
RB = 256
STEPS = KP // RB
EXACT = 2
LOG2E = 1.4426950408889634
LN2 = 0.6931471805599453
SHIFT = 65.0
NEG = -1e30
UVROWS = 24
MESH = pl.DeviceIdType.MESH
F32 = jnp.float32
BF16 = jnp.bfloat16
TRANS = (((1,), (1,)), ((), ()))


def remote(src, dst, send, recv, z, y):
    return pltpu.make_async_remote_copy(
        src_ref=src, dst_ref=dst, send_sem=send, recv_sem=recv,
        device_id={"z": z, "y": y}, device_id_type=MESH,
    )


class Gather:
    def __init__(self, cols, send, recv, z, y):
        self.cols, self.send, self.recv, self.at = cols, send, recv, (z, y)

    def where(self, route, first, second):
        return (first, second) if route == 0 else (second, first)

    def part(self, route, which):
        lo = 2 * route
        return {"both": pl.ds(lo, 2), "low": pl.ds(lo, 1), "high": pl.ds(lo + 1, 1)}[which]

    def block(self, route, which, first, second):
        z, y = self.where(route, first, second)
        return self.cols.at[self.part(route, which), z, pl.ds(pl.multiple_of(y * B, B), B), :]

    def line(self, route, which, second):
        part = self.part(route, which)
        if route == 0:
            return self.cols.at[part, :, pl.ds(pl.multiple_of(second * B, B), B), :]
        return self.cols.at[part, second, :, :]

    def copy(self, route, step, sign, k, sending):
        f, g = self.at if route == 0 else self.at[::-1]
        slot = route * 14 + {1: 0, 2: 2, 3: 4, 4: 12}[step] + (sign < 0)
        if step == 3:
            slot += 2 * k
        wrap = lambda a: lax.rem(a + 8, 4)
        if step == 1:
            ref = self.block(route, "both", f if sending else wrap(f - sign), g)
        elif step == 2:
            ref = self.block(route, "low" if sign > 0 else "high", wrap(f - sign) if sending else wrap(f + 2), g)
        elif step == 3:
            ref = self.block(route, "both", wrap(f + k), g if sending else wrap(g - sign))
        else:
            ref = self.line(route, "low" if sign > 0 else "high", wrap(g - sign) if sending else wrap(g + 2))
        if step <= 2:
            z, y = self.where(route, wrap(f + sign), g)
        else:
            z, y = self.where(route, f, wrap(g + sign))
        return remote(ref, ref, self.send.at[slot], self.recv.at[slot], z, y)

    def start(self, step, ks=(0,)):
        for k in ks:
            for route in (0, 1):
                for sign in (1, -1):
                    self.copy(route, step, sign, k, True).start()

    def arrive(self, step, ks=(0,)):
        for k in ks:
            for route in (0, 1):
                for sign in (1, -1):
                    self.copy(route, step, sign, k, False).wait_recv()

    def sent(self, step, ks=(0,)):
        for k in ks:
            for route in (0, 1):
                for sign in (1, -1):
                    self.copy(route, step, sign, k, True).wait_send()

    def point(self, number):
        if number == 0:
            self.start(1)
            self.start(3, (0,))
        elif number == 1:
            self.arrive(1)
            self.start(2)
            self.start(3, (1, 3))
        elif number == 2:
            self.arrive(2)
            self.start(3, (2,))
        elif number == 3:
            self.arrive(3, (0, 1, 3, 2))
            self.start(4)
        else:
            self.arrive(4)

    def drain(self):
        self.sent(1)
        self.sent(2)
        self.sent(3, (0, 1, 2, 3))
        self.sent(4)


def count_vector(counts, pairs, p, side):
    return jnp.full((1, 128), counts[pairs[p, side]], jnp.int32)


def lanes():
    return lax.broadcasted_iota(jnp.int32, (1, 128), 1)


def main_kernel(
    pairs, counts, bins, desc, s_out, uv_out,
    sel, own, cols, kmat, khigh, klow, ys, nus, acc, xs, xv, mv, stage, uvr, sv,
    a_send, a_recv, g_send, g_recv, u_send, u_recv, o_sem,
):
    z, y = lax.axis_index("z"), lax.axis_index("y")
    core = lax.rem(lax.axis_index("pair"), 2)
    me = z * 4 + y
    mine = pl.ds(pl.multiple_of(me * B, B), B)

    barrier = pltpu.get_barrier_semaphore()
    for other in range(1, 16):
        pl.semaphore_signal(
            barrier, inc=1, device_id_type=MESH,
            device_id={"z": lax.rem(z + other // 4, 4), "y": lax.rem(y + other % 4, 4)},
        )
    owner_y = [lax.rem(p + 2 * core, 4) for p in range(4)]
    owner = y == lax.rem(z + 2 * core, 4)

    for p in range(4):
        sel[p, 0] = desc[pairs[p, 0]]
        col = desc[pairs[p, 1]]
        sel[p, 1] = col
        cols[p, z, pl.ds(pl.multiple_of(y * B, B), B), :] = col

    @pl.when(owner)
    def _():
        own[0, mine, :] = desc[pairs[z, 0]]
        own[1, mine, :] = desc[pairs[z, 1]]

    pl.semaphore_wait(barrier, 15)

    def to_owner(p):
        there = own.at[:, mine, :]
        return remote(sel.at[p], there, a_send.at[p], a_recv.at[me], p, owner_y[p])

    for p in range(4):
        pl.when(jnp.logical_not((z == p) & (y == owner_y[p])))(lambda p=p: to_owner(p).start())
    for p in range(4):
        pl.when(jnp.logical_not((z == p) & (y == owner_y[p])))(lambda p=p: to_owner(p).wait_send())

    gather = Gather(cols, g_send, g_recv, z, y)
    gather.point(0)

    @pl.when(jnp.logical_not(owner))
    def _():
        for number in range(1, 5):
            gather.point(number)

    @pl.when(owner)
    def _():
        for source in range(16):
            def landed(source=source):
                there = own.at[:, pl.ds(source * B, B), :]
                remote(there, there, a_send.at[0], a_recv.at[source], z, y).wait_recv()
            pl.when(me != source)(landed)

        na, nb = count_vector(counts, pairs, z, 0), count_vector(counts, pairs, z, 1)
        naf, nbf = na.astype(F32), nb.astype(F32)
        one = 1.0 / (naf + nbf)
        bin_value = jnp.full((1, 128), bins[0], F32)
        bin_two = bin_value * LOG2E
        for c in range(16):
            kept = lanes() + c * 128 < nb
            nus[:, c * 128 : c * 128 + 128] = jnp.where(kept, one, 0.0)
            ys[:, c * 128 : c * 128 + 128] = jnp.where(kept, 1.0, 0.0)
        nus[:, KP:W] = jnp.where(lanes() == 0, naf * one, 0.0)
        ys[:, KP:W] = jnp.where(lanes() == 0, 1.0, 0.0)
        mu_bin = nbf * one

        def score_step(b, _):
            rows = pl.ds(pl.multiple_of(b * RB, RB), RB)
            left = own[0, rows, :]
            top = jnp.broadcast_to(bin_two, (RB, 128))
            for c in range(8):
                part = lax.dot_general(left, own[1, c * 256 : c * 256 + 256, :], TRANS, preferred_element_type=F32)
                for h in range(2):
                    at = c * 256 + h * 128
                    veil = jnp.where(lanes() + at < nb, 0.0, NEG)
                    piece = part[:, h * 128 : h * 128 + 128] * (LOG2E / 16.0) + veil
                    kmat[rows, at : at + 128] = piece
                    top = jnp.maximum(top, piece)
            top = jnp.broadcast_to(jnp.max(top, axis=1, keepdims=True), (RB, 128)) - SHIFT
            for h in range(2):
                mv[pl.ds(2 * b + h, 1), :] = top[h * 128 : h * 128 + 128].T[0:1, :]
            for c in range(CHUNKS):
                at = slice(c * 128, c * 128 + 128)
                if c < 16:
                    value = jnp.exp2(kmat[rows, at] - top)
                else:
                    value = jnp.where(lanes() == 0, jnp.exp2(bin_two - top), 0.0)
                kmat[rows, at] = value
                high = value.astype(BF16)
                khigh[rows, at] = high
                klow[rows, at] = (value - high.astype(F32)).astype(BF16)
            return 0

        lax.fori_loop(0, STEPS, score_step, 0)
        gather.point(1)

        def row_step(b):
            for h in range(2):
                rows = pl.ds(pl.multiple_of(b * RB + h * 128, 128), 128)
                total = kmat[rows, 0:128] * ys[:, 0:128]
                for c in range(1, CHUNKS):
                    total += kmat[rows, c * 128 : c * 128 + 128] * ys[:, c * 128 : c * 128 + 128]
                x = one / jnp.sum(total.T, axis=0, keepdims=True)
                xv[pl.ds(2 * b + h, 1), :] = x
                x = jnp.where(lanes() + (b * RB + h * 128) < na, x, 0.0)
                high = x.astype(BF16).astype(F32)
                line = lax.broadcasted_iota(jnp.int32, (16, 128), 0)
                both = jnp.where(line == 0, high, jnp.where(line == 1, x - high, 0.0))
                xs[lax.rem(b, 2), :, h * 128 : h * 128 + 128] = both.astype(BF16)

        def col_step(b, exact):
            rows = pl.ds(pl.multiple_of(b * RB, RB), RB)
            x = xs[lax.rem(b, 2)]
            total = jnp.dot(x, khigh[rows, :], preferred_element_type=F32)
            if exact:
                total += jnp.dot(x, klow[rows, :], preferred_element_type=F32)
            acc[...] += total

        def sweep(exact):
            spread = jnp.sum(ys[...], axis=1, keepdims=True)
            x_bin = mu_bin / jnp.broadcast_to(spread, (1, 128))
            stage[0, 17:18, :] = x_bin
            acc[...] = jnp.zeros_like(acc)
            row_step(0)

            def both(b, _):
                row_step(b)
                col_step(b - 1, exact)
                return 0

            lax.fori_loop(1, STEPS, both, 0)
            col_step(STEPS - 1, exact)
            for c in range(CHUNKS):
                at = slice(c * 128, c * 128 + 128)
                ys[:, at] = nus[:, at] / (acc[0:1, at] + acc[1:2, at] + x_bin)

        def early(i, _):
            sweep(False)
            pl.when(i == 2)(lambda: gather.point(2))
            pl.when(i == 5)(lambda: gather.point(3))
            return 0

        lax.fori_loop(0, ITERS - EXACT, early, 0)
        lax.fori_loop(0, EXACT, lambda i, _: (sweep(True), 0)[1], 0)

        u = jnp.log(xv[...]) - mv[...] * LN2
        u_bin = jnp.log(stage[0, 17:18, :]) - bin_value
        v = [jnp.log(ys[:, c * 128 : c * 128 + 128]) for c in range(16)]
        v_bin = jnp.log(jnp.broadcast_to(ys[:, KP : KP + 1], (1, 128)))
        for d in range(16):
            for c in range(16):
                stage[d, c : c + 1, :] = v[c]
            stage[d, 16:17, :] = u[d : d + 1, :]
            stage[d, 17:18, :] = u_bin
            stage[d, 18:19, :] = v_bin
            stage[d, 19:24, :] = jnp.zeros((5, 128), F32)

        uvr[z] = stage[me]
        for d in range(16):
            def send(d=d):
                remote(stage.at[d], uvr.at[z], u_send.at[d], u_recv.at[z], d // 4, d % 4).start()
            pl.when(me != d)(send)
        gather.point(4)

    for p in range(4):
        for c in range(8):
            part = lax.dot_general(
                sel[p, 0], cols[p, c // 2, (c % 2) * 256 : (c % 2) * 256 + 256, :], TRANS, preferred_element_type=F32
            )
            sv[p, :, c * 256 : c * 256 + 256] = part * 0.0625
        pltpu.make_async_copy(sv.at[p], s_out.at[p], o_sem.at[p]).start()
    gather.drain()
    for p in range(4):
        def landed(p=p):
            remote(uvr.at[p], uvr.at[p], u_send.at[0], u_recv.at[p], z, y).wait_recv()
        pl.when(jnp.logical_not((z == p) & (y == owner_y[p])))(landed)
    uv_out[...] = uvr[...]

    @pl.when(owner)
    def _():
        for d in range(16):
            def gone(d=d):
                remote(stage.at[d], uvr.at[z], u_send.at[d], u_recv.at[z], d // 4, d % 4).wait_send()
            pl.when(me != d)(gone)

    for p in range(4):
        pltpu.make_async_copy(sv.at[p], s_out.at[p], o_sem.at[p]).wait()


def last_kernel(pairs, counts, bins, s, uv, out, row_out, col_out):
    p = pl.program_id(0)
    start = (lax.axis_index("z") * 4 + lax.axis_index("y")) * B
    na, nb = count_vector(counts, pairs, p, 0), count_vector(counts, pairs, p, 1)
    norm = -jnp.log((na + nb).astype(F32))
    bin_value = jnp.full((1, 128), bins[0], F32)
    u = uv[p, 16:17, :]
    row_kept = lanes() + start < na
    u_down = jnp.broadcast_to(u, (B, 128)).T
    kept = lax.broadcasted_iota(jnp.int32, (B, 128), 0) + start < na
    for c in range(16):
        at = slice(c * 128, c * 128 + 128)
        v = uv[p, c : c + 1, :]
        col_kept = lanes() + c * 128 < nb
        out[0, :, at] = jnp.where(kept & col_kept, s[0, :, at] + u_down + v - norm, 0.0)

    def bin_lines(q):
        row_out[q : q + 1, :] = jnp.where(row_kept, bin_value + u + uv[p, 18:19, :] - norm, 0.0)
        for c in range(16):
            line = bin_value + uv[p, 17:18, :] + uv[p, c : c + 1, :] - norm
            col_out[q : q + 1, c * 128 : c * 128 + 128] = jnp.where(lanes() + c * 128 < nb, line, 0.0)

    for q in range(4):
        pl.when(p == q)(lambda q=q: bin_lines(q))


def on_device(descriptors, counts, pairs, bin_score):
    smem = pl.BlockSpec(memory_space=pltpu.SMEM)
    vmem = pl.BlockSpec(memory_space=pltpu.VMEM)
    dma = pltpu.SemaphoreType.DMA
    s, uv = pl.pallas_call(
        main_kernel,
        out_shape=(
            jax.ShapeDtypeStruct((4, B, KP), F32),
            jax.ShapeDtypeStruct((4, UVROWS, 128), F32),
        ),
        in_specs=[smem, smem, smem, vmem],
        out_specs=(pl.BlockSpec(memory_space=pl.ANY), vmem),
        scratch_shapes=[
            pltpu.VMEM((4, 2, B, D), BF16),
            pltpu.VMEM((2, KP, D), BF16),
            pltpu.VMEM((4, 4, 4 * B, D), BF16),
            pltpu.VMEM((KP, W), F32),
            pltpu.VMEM((KP, W), BF16),
            pltpu.VMEM((KP, W), BF16),
            pltpu.VMEM((1, W), F32),
            pltpu.VMEM((1, W), F32),
            pltpu.VMEM((16, W), F32),
            pltpu.VMEM((2, 16, RB), BF16),
            pltpu.VMEM((16, 128), F32),
            pltpu.VMEM((16, 128), F32),
            pltpu.VMEM((16, UVROWS, 128), F32),
            pltpu.VMEM((4, UVROWS, 128), F32),
            pltpu.VMEM((4, B, KP), F32),
            dma((4,)), dma((16,)), dma((28,)), dma((28,)), dma((16,)), dma((4,)), dma((4,)),
        ],
        compiler_params=pltpu.CompilerParams(
            collective_id=0, has_side_effects=True, vmem_limit_bytes=60 * 1024 * 1024
        ),
        name="match",
    )(pairs, counts, bin_score, descriptors)
    return pl.pallas_call(
        last_kernel,
        grid=(4,),
        out_shape=(
            jax.ShapeDtypeStruct((4, B, KP), F32),
            jax.ShapeDtypeStruct((4, B), F32),
            jax.ShapeDtypeStruct((4, KP), F32),
        ),
        in_specs=[
            smem, smem, smem,
            pl.BlockSpec((1, B, KP), lambda p: (p, 0, 0)),
            pl.BlockSpec((4, UVROWS, 128), lambda p: (0, 0, 0)),
        ],
        out_specs=(
            pl.BlockSpec((1, B, KP), lambda p: (p, 0, 0)),
            pl.BlockSpec((4, B), lambda p: (0, 0)),
            pl.BlockSpec((4, KP), lambda p: (0, 0)),
        ),
        name="assign",
    )(pairs, counts, bin_score, s, uv)


def solution(mesh):
    finer = Mesh(mesh.devices.reshape(mesh.shape["pair"], 4, 4), ("pair", "z", "y"))
    row = ("z", "y")
    return jax.shard_map(
        on_device,
        mesh=finer,
        in_specs=(P("pair", row, None), P("pair"), P("pair", None), P()),
        out_specs=(P("pair", row, None), P("pair", row), P("pair", None)),
        check_vma=False,
    )
```

```python
import contextlib

import jax
import jax.numpy as jnp
from jax import lax
from jax.experimental import pallas as pl
from jax.experimental.pallas import tpu as pltpu
from jax.sharding import Mesh
from jax.sharding import PartitionSpec as P

D = 256
ITERS = 10
KP = 2048
B = 128
W = KP + 128
CHUNKS = W // 128
RB = 256
STEPS = KP // RB
EXACT = 2
LOG2E = 1.4426950408889634
LN2 = 0.6931471805599453
SHIFT = 65.0
NEG = -1e30
UVROWS = 24
MESH = pl.DeviceIdType.MESH
SCOPES = False
EAGER = True
F32 = jnp.float32
BF16 = jnp.bfloat16
TRANS = (((1,), (1,)), ((), ()))


def scope(name):
    return jax.named_scope(name) if SCOPES else contextlib.nullcontext()


def remote(src, dst, send, recv, z, y):
    return pltpu.make_async_remote_copy(
        src_ref=src, dst_ref=dst, send_sem=send, recv_sem=recv,
        device_id={"z": z, "y": y}, device_id_type=MESH,
    )


class Gather:
    def __init__(self, cols, send, recv, z, y):
        self.cols, self.send, self.recv, self.at = cols, send, recv, (z, y)

    def where(self, route, first, second):
        return (first, second) if route == 0 else (second, first)

    def part(self, route, which):
        lo = 2 * route
        return {"both": pl.ds(lo, 2), "low": pl.ds(lo, 1), "high": pl.ds(lo + 1, 1)}[which]

    def block(self, route, which, first, second):
        z, y = self.where(route, first, second)
        return self.cols.at[self.part(route, which), z, pl.ds(pl.multiple_of(y * B, B), B), :]

    def line(self, route, which, second):
        part = self.part(route, which)
        if route == 0:
            return self.cols.at[part, :, pl.ds(pl.multiple_of(second * B, B), B), :]
        return self.cols.at[part, second, :, :]

    def copy(self, route, step, sign, k, sending):
        f, g = self.at if route == 0 else self.at[::-1]
        slot = route * 14 + {1: 0, 2: 2, 3: 4, 4: 12}[step] + (sign < 0)
        if step == 3:
            slot += 2 * k
        wrap = lambda a: lax.rem(a + 8, 4)
        if step == 1:
            ref = self.block(route, "both", f if sending else wrap(f - sign), g)
        elif step == 2:
            ref = self.block(route, "low" if sign > 0 else "high", wrap(f - sign) if sending else wrap(f + 2), g)
        elif step == 3:
            ref = self.block(route, "both", wrap(f + k), g if sending else wrap(g - sign))
        else:
            ref = self.line(route, "low" if sign > 0 else "high", wrap(g - sign) if sending else wrap(g + 2))
        if step <= 2:
            z, y = self.where(route, wrap(f + sign), g)
        else:
            z, y = self.where(route, f, wrap(g + sign))
        return remote(ref, ref, self.send.at[slot], self.recv.at[slot], z, y)

    def start(self, step, ks=(0,)):
        for k in ks:
            for route in (0, 1):
                for sign in (1, -1):
                    self.copy(route, step, sign, k, True).start()

    def arrive(self, step, ks=(0,)):
        for k in ks:
            for route in (0, 1):
                for sign in (1, -1):
                    self.copy(route, step, sign, k, False).wait_recv()

    def sent(self, step, ks=(0,)):
        for k in ks:
            for route in (0, 1):
                for sign in (1, -1):
                    self.copy(route, step, sign, k, True).wait_send()

    def point(self, number):
        if number == 0:
            self.start(1)
            self.start(3, (0,))
        elif number == 1:
            self.arrive(1)
            self.start(2)
            self.start(3, (1, 3))
        elif number == 2:
            self.arrive(2)
            self.start(3, (2,))
        elif number == 3:
            self.arrive(3, (0, 1, 3, 2))
            self.start(4)
        else:
            self.arrive(4)

    def drain(self):
        self.sent(1)
        self.sent(2)
        self.sent(3, (0, 1, 2, 3))
        self.sent(4)


def count_vector(counts, pairs, p, side):
    return jnp.full((1, 128), counts[pairs[side, p]], jnp.int32)


def lanes():
    return lax.broadcasted_iota(jnp.int32, (1, 128), 1)


NEAR = (
    (0, 0), (0, 1), (0, 3), (1, 0), (3, 0), (1, 1), (1, 3), (3, 1), (3, 3), (0, 2), (2, 0), (1, 2), (3, 2), (2, 1), (2, 3), (2, 2),
)


def main_kernel(
    pairs, counts, bins, desc, s_out, uv_out,
    sel, own, cols, kmat, khigh, raw0, raw1, top0, top1, ys, nus, xd, xv, mv, stage, uvr, sv,
    a_send, c_recv, r_recv, g_send, g_recv, u_send, u_recv, o_sem,
):
    z, y = lax.axis_index("z"), lax.axis_index("y")
    core = lax.rem(lax.axis_index("pair"), 2)
    me = z * 4 + y

    barrier = pltpu.get_barrier_semaphore()
    for other in range(1, 16):
        pl.semaphore_signal(
            barrier, inc=1, device_id_type=MESH,
            device_id={"z": lax.rem(z + other // 4, 4), "y": lax.rem(y + other % 4, 4)},
        )
    owner_y = [lax.rem(p + 2 * core, 4) for p in range(4)]
    owner = y == lax.rem(z + 2 * core, 4)

    with scope("select"):
        for p in range(4):
            sel[p, 0] = desc[pairs[0, p]]
            col = desc[pairs[1, p]]
            sel[p, 1] = col
            cols[p, z, pl.ds(pl.multiple_of(y * B, B), B), :] = col

        @pl.when(owner)
        def _():
            own[0, 0] = desc[pairs[0, z]]
            own[1, 0] = desc[pairs[1, z]]

    with scope("barrier"):
        pl.semaphore_wait(barrier, 15)

    def to_owner(p, side):
        slot = lax.rem(z + 4 - p, 4) * 4 + lax.rem(y + 4 - owner_y[p], 4)
        recv = (r_recv, c_recv)[side].at[slot]
        return remote(sel.at[p, side], own.at[side, slot], a_send.at[p, side], recv, p, owner_y[p])

    away = [jnp.logical_not((z == p) & (y == owner_y[p])) for p in range(4)]
    with scope("to_owner"):
        for side in (1, 0):
            for p in range(4):
                pl.when(away[p])(lambda p=p: to_owner(p, side).start())

    gather = Gather(cols, g_send, g_recv, z, y)

    def sent():
        for side in (1, 0):
            for p in range(4):
                pl.when(away[p])(lambda p=p: to_owner(p, side).wait_send())

    def pt(number):
        with scope(f"pt{number}"):
            gather.point(number)

    def answer(h):
        dz, dy = NEAR[h]
        return remote(
            stage.at[h], uvr.at[z], u_send.at[h], u_recv.at[z], lax.rem(z + dz, 4), lax.rem(y + dy, 4)
        )

    if not EAGER:
        sent()
    pt(0)
    if EAGER:
        sent()

    @pl.when(jnp.logical_not(owner))
    def _():
        for number in range(1, 5):
            pt(number)

    @pl.when(owner)
    def _():
        def landed(side, slot):
            there = own.at[side, slot]
            remote(there, there, a_send.at[0, 0], (r_recv, c_recv)[side].at[slot], z, y).wait_recv()

        def number_of(slot):
            dz, dy = slot if isinstance(slot, tuple) else (slot // 4, slot % 4)
            return lax.rem(z + dz, 4) * 4 + lax.rem(y + dy, 4)

        na, nb = count_vector(counts, pairs, z, 0), count_vector(counts, pairs, z, 1)
        naf, nbf = na.astype(F32), nb.astype(F32)
        one = 1.0 / (naf + nbf)
        bin_value = jnp.full((1, 128), bins[0], F32)
        mu_bin = nbf * one

        with scope("landed"):
            for slot in range(1, 16):
                landed(1, slot)
            for slot in range(16):
                start = number_of(slot) * B
                kept = lanes() + start < nb
                nus[:, slot * 128 : slot * 128 + 128] = jnp.where(kept, one, 0.0)
                ys[:, slot * 128 : slot * 128 + 128] = jnp.where(kept, 1.0, 0.0)
                kept = lax.broadcasted_iota(jnp.int32, (B, D), 0) + start < jnp.concatenate([nb, nb], axis=1)
                own[1, slot] = own[1, slot] * jnp.where(kept, 1.0, 0.0).astype(BF16)
            nus[:, KP:W] = jnp.where(lanes() == 0, naf * one, 0.0)
            ys[:, KP:W] = jnp.where(lanes() == 0, 1.0, 0.0)

        def multiply(step, raw, tops):
            left = jnp.concatenate([own[0, dz * 4 + dy] for dz, dy in NEAR[2 * step : 2 * step + 2]], axis=0)
            top = jnp.broadcast_to(bin_value * 16.0, (RB, 128))
            for c in range(8):
                right = jnp.concatenate([own[1, 2 * c], own[1, 2 * c + 1]], axis=0)
                part = lax.dot_general(left, right, TRANS, preferred_element_type=F32)
                raw[:, c * 256 : c * 256 + 256] = part
                top = jnp.maximum(top, jnp.maximum(part[:, 0:128], part[:, 128:256]))
            tops[...] = top

        def scale(step, raw, tops):
            rows = slice(step * RB, step * RB + RB)
            top = jnp.max(tops[...], axis=1, keepdims=True) * (LOG2E / 16.0) - SHIFT
            top = jnp.broadcast_to(top, (RB, 128))
            for h in range(2):
                mv[2 * step + h : 2 * step + h + 1, :] = top[h * 128 : h * 128 + 128].T[0:1, :]
            for c in range(CHUNKS):
                at = slice(c * 128, c * 128 + 128)
                if c < 16:
                    value = jnp.exp2(raw[:, at] * (LOG2E / 16.0) - top)
                else:
                    value = jnp.where(lanes() == 0, jnp.exp2(bin_value * LOG2E - top), 0.0)
                kmat[rows, at] = value
                khigh[c, rows, :] = value.astype(BF16)

        with scope("scores"):
            raws = ((raw0, top0), (raw1, top1))
            for step in range(STEPS):
                for dz, dy in NEAR[2 * step : 2 * step + 2]:
                    if dz or dy:
                        landed(0, dz * 4 + dy)
                if step == 2:
                    pt(1)
                if step:
                    scale(step - 1, *raws[(step - 1) % 2])
                multiply(step, *raws[step % 2])
            scale(STEPS - 1, *raws[(STEPS - 1) % 2])

        def weigh(h):
            rows = slice(h * 128, h * 128 + 128)
            total = kmat[rows, 0:128] * ys[:, 0:128]
            for c in range(1, CHUNKS):
                total += kmat[rows, c * 128 : c * 128 + 128] * ys[:, c * 128 : c * 128 + 128]
            return total

        def across(h, total):
            x = one / jnp.sum(total.T, axis=0, keepdims=True)
            xv[h : h + 1, :] = x
            return jnp.where(lanes() + number_of(NEAR[h]) * B < na, x, 0.0)

        def bins_row():
            spread = jnp.sum(ys[...], axis=1, keepdims=True)
            x_bin = mu_bin / jnp.broadcast_to(spread, (1, 128))
            stage[0, 17:18, :] = x_bin
            return x_bin

        def early():
            x_bin = bins_row()
            line = lax.broadcasted_iota(jnp.int32, (16, 128), 0)
            sums = [None] * 9

            def row_step(b):
                halves = []
                for h in (2 * b, 2 * b + 1):
                    x = across(h, weigh(h))
                    high = x.astype(BF16).astype(F32)
                    halves.append(jnp.where(line == 0, high, jnp.where(line == 1, x - high, 0.0)).astype(BF16))
                return jnp.concatenate(halves, axis=1)

            def col_step(b, x):
                rows = slice(b * RB, b * RB + RB)
                for t in range(9):
                    chunks = [khigh[c, rows, :] for c in range(2 * t, min(2 * t + 2, CHUNKS))]
                    part = jnp.dot(x, jnp.concatenate(chunks, axis=1), preferred_element_type=F32)
                    sums[t] = part if b == 0 else sums[t] + part

            x = row_step(0)
            for b in range(1, STEPS):
                after = row_step(b)
                col_step(b - 1, x)
                x = after
            col_step(STEPS - 1, x)
            for t in range(9):
                at = slice(t * 256, min(t * 256 + 256, W))
                both = sums[t][0:1, :] + sums[t][1:2, :]
                ys[:, at] = nus[:, at] / (both + x_bin[:, 0:1])

        def late():
            x_bin = bins_row()

            def row_step(h):
                total = weigh(h)
                across(h, total)
                x = one / jnp.broadcast_to(jnp.sum(total, axis=1, keepdims=True), (B, 128))
                kept = lax.broadcasted_iota(jnp.int32, (B, 128), 0) + number_of(NEAR[h]) * B < na
                xd[h % 2] = jnp.where(kept, x, 0.0)

            sums = [jnp.zeros((8, 128), F32)] * CHUNKS

            def col_step(h):
                for c in range(CHUNKS):
                    part = kmat[h * 128 : h * 128 + 128, c * 128 : c * 128 + 128] * xd[h % 2]
                    sums[c] = sums[c] + jnp.sum(part.reshape(16, 8, 128), axis=0)

            row_step(0)
            for h in range(1, 16):
                row_step(h)
                col_step(h - 1)
            col_step(15)
            for c in range(CHUNKS):
                at = slice(c * 128, c * 128 + 128)
                ys[:, at] = nus[:, at] / (jnp.sum(sums[c], axis=0, keepdims=True) + x_bin)

        def early_sweep(i, _):
            with scope("sweep"):
                early()
            pl.when(i == 0)(lambda: pt(2))
            pl.when(i == 4)(lambda: pt(3))
            return 0

        lax.fori_loop(0, ITERS - EXACT, early_sweep, 0)

        def late_sweep(i, _):
            with scope("exact"):
                late()
            return 0

        lax.fori_loop(0, EXACT, late_sweep, 0)

        with scope("uv"):
            u = jnp.log(xv[...]) - mv[...] * LN2
            u_bin = jnp.log(stage[0, 17:18, :]) - bin_value
            v = [jnp.log(ys[:, c * 128 : c * 128 + 128]) for c in range(16)]
            v_bin = jnp.log(jnp.broadcast_to(ys[:, KP : KP + 1], (1, 128)))
            for h in range(16):
                d = number_of(NEAR[h])
                for c in range(16):
                    stage[h, pl.ds(number_of(c), 1), :] = v[c]
                stage[h, 16:17, :] = u[h : h + 1, :]
                stage[h, 17:18, :] = u_bin
                stage[h, 18:19, :] = v_bin
                stage[h, 19:24, :] = jnp.zeros((5, 128), F32)

            uvr[z] = stage[0]
            for h in range(1, 16):
                answer(h).start()

        pt(4)

    with scope("final"):
        for p in range(4):
            for c in range(8):
                right = cols[p, c // 2, (c % 2) * 256 : (c % 2) * 256 + 256, :]
                part = lax.dot_general(sel[p, 0], right, TRANS, preferred_element_type=F32)
                sv[p, :, c * 256 : c * 256 + 256] = part * 0.0625
            pltpu.make_async_copy(sv.at[p], s_out.at[p], o_sem.at[p]).start()

    with scope("drain"):
        gather.drain()

    with scope("uvwait"):
        for p in range(4):
            def landed(p=p):
                remote(uvr.at[p], uvr.at[p], u_send.at[0], u_recv.at[p], z, y).wait_recv()
            pl.when(away[p])(landed)

    uv_out[...] = uvr[...]

    @pl.when(owner)
    def _():
        for h in range(1, 16):
            answer(h).wait_send()

    for p in range(4):
        pltpu.make_async_copy(sv.at[p], s_out.at[p], o_sem.at[p]).wait()


def last_kernel(pairs, counts, bins, s, uv, out, row_out, col_out):
    p = pl.program_id(0)
    start = (lax.axis_index("z") * 4 + lax.axis_index("y")) * B
    na, nb = count_vector(counts, pairs, p, 0), count_vector(counts, pairs, p, 1)
    norm = -jnp.log((na + nb).astype(F32))
    bin_value = jnp.full((1, 128), bins[0], F32)
    u = uv[p, 16:17, :]
    row_kept = lanes() + start < na
    u_down = jnp.broadcast_to(u, (B, 128)).T
    kept = lax.broadcasted_iota(jnp.int32, (B, 128), 0) + start < na
    for c in range(16):
        at = slice(c * 128, c * 128 + 128)
        v = uv[p, c : c + 1, :]
        col_kept = lanes() + c * 128 < nb
        out[0, :, at] = jnp.where(kept & col_kept, s[0, :, at] + u_down + v - norm, 0.0)

    def bin_lines(q):
        row_out[q : q + 1, :] = jnp.where(row_kept, bin_value + u + uv[p, 18:19, :] - norm, 0.0)
        for c in range(16):
            line = bin_value + uv[p, 17:18, :] + uv[p, c : c + 1, :] - norm
            col_out[q : q + 1, c * 128 : c * 128 + 128] = jnp.where(lanes() + c * 128 < nb, line, 0.0)

    for q in range(4):
        pl.when(p == q)(lambda q=q: bin_lines(q))


def on_device(descriptors, counts, pairs, bin_score):
    smem = pl.BlockSpec(memory_space=pltpu.SMEM)
    vmem = pl.BlockSpec(memory_space=pltpu.VMEM)
    dma = pltpu.SemaphoreType.DMA
    s, uv = pl.pallas_call(
        main_kernel,
        out_shape=(
            jax.ShapeDtypeStruct((4, B, KP), F32),
            jax.ShapeDtypeStruct((4, UVROWS, 128), F32),
        ),
        in_specs=[smem, smem, smem, vmem],
        out_specs=(pl.BlockSpec(memory_space=pl.ANY), vmem),
        scratch_shapes=[
            pltpu.VMEM((4, 2, B, D), BF16),
            pltpu.VMEM((2, 16, B, D), BF16),
            pltpu.VMEM((4, 4, 4 * B, D), BF16),
            pltpu.VMEM((KP, W), F32),
            pltpu.VMEM((CHUNKS, KP, 128), BF16),
            pltpu.VMEM((RB, KP), F32),
            pltpu.VMEM((RB, KP), F32),
            pltpu.VMEM((RB, 128), F32),
            pltpu.VMEM((RB, 128), F32),
            pltpu.VMEM((1, W), F32),
            pltpu.VMEM((1, W), F32),
            pltpu.VMEM((2, B, 128), F32),
            pltpu.VMEM((16, 128), F32),
            pltpu.VMEM((16, 128), F32),
            pltpu.VMEM((16, UVROWS, 128), F32),
            pltpu.VMEM((4, UVROWS, 128), F32),
            pltpu.VMEM((4, B, KP), F32),
            dma((4, 2)), dma((16,)), dma((16,)), dma((28,)), dma((28,)), dma((16,)), dma((4,)), dma((4,)),
        ],
        compiler_params=pltpu.CompilerParams(
            collective_id=0, has_side_effects=True, vmem_limit_bytes=60 * 1024 * 1024
        ),
        name="match",
    )(pairs.T, counts, bin_score, descriptors)
    return pl.pallas_call(
        last_kernel,
        grid=(4,),
        out_shape=(
            jax.ShapeDtypeStruct((4, B, KP), F32),
            jax.ShapeDtypeStruct((4, B), F32),
            jax.ShapeDtypeStruct((4, KP), F32),
        ),
        in_specs=[
            smem, smem, smem,
            pl.BlockSpec((1, B, KP), lambda p: (p, 0, 0)),
            pl.BlockSpec((4, UVROWS, 128), lambda p: (0, 0, 0)),
        ],
        out_specs=(
            pl.BlockSpec((1, B, KP), lambda p: (p, 0, 0)),
            pl.BlockSpec((4, B), lambda p: (0, 0)),
            pl.BlockSpec((4, KP), lambda p: (0, 0)),
        ),
        name="assign",
    )(pairs.T, counts, bin_score, s, uv)


def solution(mesh):
    finer = Mesh(mesh.devices.reshape(mesh.shape["pair"], 4, 4), ("pair", "z", "y"))
    row = ("z", "y")
    return jax.shard_map(
        on_device,
        mesh=finer,
        in_specs=(P("pair", row, None), P("pair"), P("pair", None), P()),
        out_specs=(P("pair", row, None), P("pair", row), P("pair", None)),
        check_vma=False,
    )
```
